128 devices in a mesh: terms: 128 (over z, y, x, core).
Axes of the slice: x: 4, y: 4, z: 4, core: 2. Of those that a mesh axis runs over, the one named last changes fastest.
Arguments:
- psi: float32 [3, 128, 4, 4, 128], replicated
- left_env: bfloat16 [3072, 128, 128], P('terms')
- phys_op: bfloat16 [3072, 16, 16], P('terms')
- right_env: bfloat16 [3072, 128, 128], P('terms')
Outputs:
- output 1: float32 [3, 7, 128, 4, 4, 128], P(None, None, 'terms')
- output 2: float32 [3, 6], replicated
- output 3: float32 [3, 6], replicated
All inputs are finite; a program needn't handle non-finite values.
Results may differ from the reference program's by a relative error of at most 0.0113775.
Values are sent between devices in bfloat16 or wider.
A program may use at most 1 GiB of HBM per device.

```python
import jax
import jax.numpy as jnp
from jax import lax

BOND_DIM = 128
PHYS_DIM = 4
ROOT_COUNT = 3
TERM_COUNT = 3072
LANCZOS_STEPS = 6
PAIRS = PHYS_DIM * PHYS_DIM
N_ELEMS = BOND_DIM * PAIRS * BOND_DIM


def symmetric_terms(key, count, width):
    noise_key, shift_key = jax.random.split(key)
    raw = jax.random.normal(noise_key, (count, width, width), jnp.float32)
    noise = (raw + jnp.swapaxes(raw, 1, 2)) * (2.0 * width) ** -0.5
    shift = jax.random.normal(shift_key, (count,), jnp.float32)
    return noise + shift[:, None, None] * jnp.eye(width, dtype=jnp.float32)


def setup_inputs(seed: int = 0) -> dict:
    keys = jax.random.split(jax.random.key(seed), 4)
    psi = jax.random.normal(keys[0], (ROOT_COUNT, BOND_DIM, PHYS_DIM, PHYS_DIM, BOND_DIM), jnp.float32)
    left_env = symmetric_terms(keys[1], TERM_COUNT, BOND_DIM).astype(jnp.bfloat16)
    phys_op = (symmetric_terms(keys[2], TERM_COUNT, PAIRS) * TERM_COUNT ** -0.5).astype(jnp.bfloat16)
    right_env = symmetric_terms(keys[3], TERM_COUNT, BOND_DIM).astype(jnp.bfloat16)
    return {'psi': psi, 'left_env': left_env, 'phys_op': phys_op, 'right_env': right_env}


def reference(psi, left_env, phys_op, right_env):
    psi_mat = psi.reshape(ROOT_COUNT, BOND_DIM, PAIRS, BOND_DIM)
    norms = jnp.sqrt(jnp.sum(psi_mat * psi_mat, axis=(1, 2, 3)) / N_ELEMS)
    v_start = psi_mat / norms[:, None, None, None]

    def matvec(v_cur):
        flat_in = v_cur.astype(jnp.bfloat16).reshape(ROOT_COUNT * BOND_DIM * PAIRS, BOND_DIM)

        def add_term(acc, term):
            left_k, phys_k, right_k = term
            right_part = jnp.dot(flat_in, right_k.T, preferred_element_type=jnp.float32).astype(jnp.bfloat16)
            right_part = right_part.reshape(ROOT_COUNT, BOND_DIM, PAIRS, BOND_DIM)
            mid_part = jnp.einsum('qu,rcub->rcqb', phys_k.astype(jnp.float32), right_part.astype(jnp.float32)).astype(jnp.bfloat16)
            left_part = jnp.einsum('ac,rcqb->raqb', left_k.astype(jnp.float32), mid_part.astype(jnp.float32))
            return acc + left_part, None

        zero_acc = jnp.zeros((ROOT_COUNT, BOND_DIM, PAIRS, BOND_DIM), jnp.float32)
        total, _ = lax.scan(add_term, zero_acc, (left_env, phys_op, right_env))
        return total

    def lanczos_step(carry, unused):
        v_prev, v_cur, beta_prev = carry
        sigma = matvec(v_cur)
        alpha = jnp.sum(sigma * v_cur, axis=(1, 2, 3)) / N_ELEMS
        residual = sigma - alpha[:, None, None, None] * v_cur - beta_prev[:, None, None, None] * v_prev
        beta = jnp.sqrt(jnp.sum(residual * residual, axis=(1, 2, 3)) / N_ELEMS)
        v_next = residual / beta[:, None, None, None]
        return (v_cur, v_next, beta), (v_next, alpha, beta)

    start_carry = (jnp.zeros_like(v_start), v_start, jnp.zeros((ROOT_COUNT,), jnp.float32))
    _, (later, alphas, betas) = lax.scan(lanczos_step, start_carry, None, length=LANCZOS_STEPS)
    vectors = jnp.concatenate([v_start[None], later], axis=0)
    vectors = jnp.transpose(vectors, (1, 0, 2, 3, 4)).reshape(ROOT_COUNT, LANCZOS_STEPS + 1, BOND_DIM, PHYS_DIM, PHYS_DIM, BOND_DIM)
    return (vectors, alphas.T, betas.T)
```

```python
import functools

import jax
import jax.numpy as jnp
from jax import lax
from jax.experimental import pallas as pl
from jax.experimental.pallas import tpu as pltpu
from jax.sharding import PartitionSpec as P

LANCZOS_STEPS = 6
MESH = pl.DeviceIdType.MESH
F32 = jnp.float32
BF16 = jnp.bfloat16
ITERS = 6


def lanczos_kernel(topo, steps, psi_ref, left_ref, phys_ref, right_ref, vec_ref, alpha_ref, beta_ref,
                   v, u, wide, za, zb, acc, wbuf, rc, rx, ry, rz, beta_prev, send_sem, recv_sem):
    nz, ny, nx, nc = topo
    roots, rows = psi_ref.shape[0], psi_ref.shape[1]
    bond = psi_ref.shape[2]
    pairs = rows // bond
    n_elems = rows * bond
    terms = left_ref.shape[0]
    me = lax.axis_index('terms')
    c = lax.rem(me, nc)
    x = lax.rem(me // nc, nx)
    y = lax.rem(me // (nc * nx), ny)
    z = me // (nc * nx * ny)
    rows_c, rows_x = rows // nc, rows // (nc * nx)
    rows_y, rows_z = rows // (nc * nx * ny), rows // (nc * nx * ny * nz)
    base_c = c * rows_c
    base_x = base_c + x * rows_x
    base_y = base_x + y * rows_y
    base_z = base_y + z * rows_z

    def device(zz, yy, xx, cc):
        return ((zz * ny + yy) * nx + xx) * nc + cc

    def hop(axis, d):
        if axis == 'c':
            cc = lax.rem(c + d, nc)
            return device(z, y, x, cc), cc
        if axis == 'x':
            xx = lax.rem(x + d, nx)
            return device(z, y, xx, c), xx
        if axis == 'y':
            yy = lax.rem(y + d, ny)
            return device(z, yy, x, c), yy
        zz = lax.rem(z + d, nz)
        return device(zz, y, x, c), zz

    sizes = {'c': nc, 'x': nx, 'y': ny, 'z': nz}
    scatter = {'c': (0, 0, rows_c, rc, 0), 'x': (base_c, 1, rows_x, rx, 1), 'y': (base_x, 2, rows_y, ry, 4),
               'z': (base_y, 3, rows_z, rz, 7)}
    gather = {'z': (base_z, rows_z, 10), 'y': (base_y, rows_y, 13), 'x': (base_x, rows_x, 16), 'c': (base_c, rows_c, 19)}

    def scatter_copies(r, axis):
        start, _, count, buf, sem0 = scatter[axis]
        out = []
        for d in range(1, sizes[axis]):
            dev, coord = hop(axis, d)
            out.append(pltpu.make_async_remote_copy(
                src_ref=acc.at[r, pl.ds(pl.multiple_of(start + coord * count, 8), count)],
                dst_ref=buf.at[r, d - 1],
                send_sem=send_sem.at[r, sem0 + d - 1], recv_sem=recv_sem.at[r, sem0 + d - 1],
                device_id=(dev,), device_id_type=MESH))
        return out

    def gather_copies(r, axis):
        start, count, sem0 = gather[axis]
        out = []
        for d in range(1, sizes[axis]):
            dev, _ = hop(axis, d)
            block = wbuf.at[r, pl.ds(pl.multiple_of(start, 8), count)]
            out.append(pltpu.make_async_remote_copy(
                src_ref=block, dst_ref=block,
                send_sem=send_sem.at[r, sem0 + d - 1], recv_sem=recv_sem.at[r, sem0 + d - 1],
                device_id=(dev,), device_id_type=MESH))
        return out

    def start(copies):
        for copy in copies:
            copy.start()

    def wait(copies):
        for copy in copies:
            copy.wait_send()
        for copy in copies:
            copy.wait_recv()

    own = {'c': base_c, 'x': base_x, 'y': base_y, 'z': base_z}

    def reduce_own(r, axis):
        _, _, count, buf, _ = scatter[axis]
        chunk = min(count, 128)

        def body(i, carry):
            at = pl.ds(pl.multiple_of(own[axis] + i * chunk, 8), chunk)
            inside = pl.ds(pl.multiple_of(i * chunk, 8), chunk)
            total = acc[r, at, :]
            for d in range(sizes[axis] - 1):
                total = total + buf[r, d, inside, :]
            if axis == 'z':
                wbuf[r, at, :] = total
            else:
                acc[r, at, :] = total
            return carry

        lax.fori_loop(0, count // chunk, body, 0)

    barrier = pltpu.get_barrier_semaphore()
    peers = [hop(axis, d)[0] for axis in 'cxyz' for d in range(1, sizes[axis])]
    for dev in peers:
        pl.semaphore_signal(barrier, inc=1, device_id=(dev,), device_id_type=MESH)
    pl.semaphore_wait(barrier, len(peers))

    big = pairs * 16
    row = lax.broadcasted_iota(jnp.int32, (big, pairs), 0) // 16
    spread = jnp.where(row == lax.broadcasted_iota(jnp.int32, (big, pairs), 1), 1.0, 0.0).astype(BF16)
    col = lax.broadcasted_iota(jnp.int32, (pairs, big), 1) // 16
    spread_t = jnp.where(col == lax.broadcasted_iota(jnp.int32, (pairs, big), 0), 1.0, 0.0).astype(BF16)
    diagonal = (lax.rem(lax.broadcasted_iota(jnp.int32, (big, big), 0), 16)
                == lax.rem(lax.broadcasted_iota(jnp.int32, (big, big), 1), 16))

    def expand(k, carry):
        tall = jnp.dot(spread, phys_ref[k], preferred_element_type=F32).astype(BF16)
        full = jnp.dot(tall, spread_t, preferred_element_type=F32)
        wide[k] = jnp.where(diagonal, full, 0.0).astype(BF16)
        return carry

    lax.fori_loop(0, terms, expand, 0)

    chunk = 2 * bond
    chunks = rows // chunk

    def fold(t):
        return jnp.sum(t.reshape(chunk // 8, 8, bond), axis=0)

    def total(t):
        return jnp.sum(t, axis=(0, 1), keepdims=True)

    def put_vector(r, nxt, i, part):
        v[r, nxt, pl.ds(pl.multiple_of(i * chunk, 8), chunk), :] = part
        u[r, pl.ds(2 * i, 2)] = part.reshape(2, bond, bond).astype(BF16)

    def put_row(r, nxt, j):
        vec_ref[r, j] = v[r, nxt, pl.ds(me, pairs, stride=bond), :]

    def first_vector(r, carry):
        def norm_body(i, s):
            part = psi_ref[r, pl.ds(pl.multiple_of(i * chunk, 8), chunk), :]
            return s + fold(part * part)

        norm = jnp.sqrt(total(lax.fori_loop(0, chunks, norm_body, jnp.zeros((8, bond), F32))) / n_elems)

        def scale_body(i, s):
            at = pl.ds(pl.multiple_of(i * chunk, 8), chunk)
            put_vector(r, 0, i, psi_ref[r, at, :] / norm)
            v[r, 1, at, :] = jnp.zeros((chunk, bond), F32)
            return s

        lax.fori_loop(0, chunks, scale_body, 0)
        beta_prev[r] = jnp.zeros((8, bond), F32)
        put_row(r, 0, 0)
        return carry

    lax.fori_loop(0, roots, first_vector, 0)

    def update(r, j):
        cur, nxt = lax.rem(j, 2), lax.rem(j + 1, 2)
        rowsof = lambda i: pl.ds(pl.multiple_of(i * chunk, 8), chunk)

        def alpha_body(i, s):
            return s + fold(wbuf[r, rowsof(i), :] * v[r, cur, rowsof(i), :])

        alpha = total(lax.fori_loop(0, chunks, alpha_body, jnp.zeros((8, bond), F32))) / n_elems
        before = beta_prev[r][0:1, 0:1]

        def residual_body(i, s):
            at = rowsof(i)
            res = wbuf[r, at, :] - alpha * v[r, cur, at, :] - before * v[r, nxt, at, :]
            wbuf[r, at, :] = res
            return s + fold(res * res)

        beta = jnp.sqrt(total(lax.fori_loop(0, chunks, residual_body, jnp.zeros((8, bond), F32))) / n_elems)

        def next_body(i, s):
            put_vector(r, nxt, i, wbuf[r, rowsof(i), :] / beta)
            return s

        lax.fori_loop(0, chunks, next_body, 0)
        alpha_ref[r, j] = jnp.broadcast_to(alpha, (8, bond))
        beta_ref[r, j] = jnp.broadcast_to(beta, (8, bond))
        beta_prev[r] = jnp.broadcast_to(beta, (8, bond))
        put_row(r, nxt, j + 1)

    def right_mid(r, p, dst):
        rp = jnp.concatenate([right_ref[2 * p], right_ref[2 * p + 1]], axis=1)
        for g2 in range(bond // 32):
            ys = []
            for g in (2 * g2, 2 * g2 + 1):
                lhs = u[r, :, g * 16:(g + 1) * 16, :].reshape(big, bond)
                ys.append(jnp.dot(lhs, rp, preferred_element_type=F32).astype(BF16))
            for k in range(2):
                rhs = jnp.concatenate([t[:, k * bond:(k + 1) * bond] for t in ys], axis=1)
                out = jnp.dot(wide[2 * p + k], rhs, preferred_element_type=F32).astype(BF16)
                for h in range(2):
                    g = 2 * g2 + h
                    dst[k, :, g * 16:(g + 1) * 16, :] = out[:, h * bond:(h + 1) * bond].reshape(pairs, 16, bond)

    def left(r, p, first):
        lp = jnp.concatenate([left_ref[2 * p + k] for k in range(4)], axis=1)
        for qp in range(pairs // 2):
            cols = []
            for q in (2 * qp, 2 * qp + 1):
                cols.append(jnp.concatenate([za[0, q], za[1, q], zb[0, q], zb[1, q]], axis=0))
            out = jnp.dot(lp, jnp.concatenate(cols, axis=1), preferred_element_type=F32)
            for h in range(2):
                q = 2 * qp + h
                at = pl.ds(q * bond, bond)
                acc[r, at, :] += out[:, h * bond:(h + 1) * bond]

    per_iter = terms // ITERS

    slots = roots * steps

    def slot(s, carry):
        r = lax.rem(s, roots)
        r1 = lax.rem(s + roots - 1, roots)
        r2 = lax.rem(s + roots - 2, roots)
        computing = s < slots
        scattering = jnp.logical_and(s >= 1, s < slots + 1)
        gathering = s >= 2

        @pl.when(computing)
        def _():
            def clear(i, t):
                acc[r, pl.ds(pl.multiple_of(i * chunk, 8), chunk), :] = jnp.zeros((chunk, bond), F32)
                return t
            lax.fori_loop(0, chunks, clear, 0)

        def step(i, t):
            @pl.when(jnp.logical_and(gathering, i == 1))
            def _():
                wait(gather_copies(r2, 'z'))
                start(gather_copies(r2, 'y'))

            @pl.when(jnp.logical_and(gathering, i == 3))
            def _():
                wait(gather_copies(r2, 'y'))
                start(gather_copies(r2, 'x'))

            @pl.when(jnp.logical_and(scattering, i == 1))
            def _():
                wait(scatter_copies(r1, 'c'))
                reduce_own(r1, 'c')
                start(scatter_copies(r1, 'x'))

            @pl.when(jnp.logical_and(scattering, i == 4))
            def _():
                wait(scatter_copies(r1, 'x'))
                reduce_own(r1, 'x')
                start(scatter_copies(r1, 'y'))

            @pl.when(computing)
            def _():
                for m in range(per_iter // 4):
                    p = i * (per_iter // 2) + 2 * m
                    right_mid(r, p, za)
                    right_mid(r, p + 1, zb)
                    left(r, p, m == 0)
            return t

        lax.fori_loop(0, ITERS, step, 0)

        @pl.when(gathering)
        def _():
            wait(gather_copies(r2, 'x'))
            start(gather_copies(r2, 'c'))

        @pl.when(computing)
        def _():
            start(scatter_copies(r, 'c'))

        @pl.when(scattering)
        def _():
            wait(scatter_copies(r1, 'y'))
            reduce_own(r1, 'y')
            start(scatter_copies(r1, 'z'))

        @pl.when(gathering)
        def _():
            wait(gather_copies(r2, 'c'))
            update(r2, (s - 2) // roots)

        @pl.when(scattering)
        def _():
            wait(scatter_copies(r1, 'z'))
            reduce_own(r1, 'z')
            start(gather_copies(r1, 'z'))
        return carry

    lax.fori_loop(0, slots + 2, slot, 0)


def build(topo, steps, roots, bond, pairs, terms):
    nz, ny, nx, nc = topo
    rows = pairs * bond
    vm = pl.BlockSpec(memory_space=pltpu.VMEM)
    rows_c, rows_x = rows // nc, rows // (nc * nx)
    rows_y, rows_z = rows_x // ny, rows_x // (ny * nz)
    return pl.pallas_call(
        functools.partial(lanczos_kernel, topo, steps),
        out_shape=(jax.ShapeDtypeStruct((roots, steps + 1, pairs, bond), F32),
                   jax.ShapeDtypeStruct((roots, steps, 8, bond), F32),
                   jax.ShapeDtypeStruct((roots, steps, 8, bond), F32)),
        in_specs=[vm] * 4,
        out_specs=(vm, vm, vm),
        scratch_shapes=[
            pltpu.VMEM((roots, 2, rows, bond), F32),
            pltpu.VMEM((roots, pairs, bond, bond), BF16),
            pltpu.VMEM((terms, pairs * 16, pairs * 16), BF16),
            pltpu.VMEM((2, pairs, bond, bond), BF16),
            pltpu.VMEM((2, pairs, bond, bond), BF16),
            pltpu.VMEM((roots, rows, bond), F32),
            pltpu.VMEM((roots, rows, bond), F32),
            pltpu.VMEM((roots, nc - 1, rows_c, bond), F32),
            pltpu.VMEM((roots, nx - 1, rows_x, bond), F32),
            pltpu.VMEM((roots, ny - 1, rows_y, bond), F32),
            pltpu.VMEM((roots, nz - 1, rows_z, bond), F32),
            pltpu.VMEM((roots, 8, bond), F32),
            pltpu.SemaphoreType.DMA((roots, 20)),
            pltpu.SemaphoreType.DMA((roots, 20)),
        ],
        compiler_params=pltpu.CompilerParams(collective_id=0, has_side_effects=True,
                                             vmem_limit_bytes=60 * 1024 * 1024),
        name='lanczos',
    )


def solution(mesh, topo=(4, 4, 4, 2), steps=LANCZOS_STEPS):
    def device_fn(psi, left_loc, phys_loc, right_loc):
        roots, bond, phys = psi.shape[0], psi.shape[1], psi.shape[2]
        pairs = phys * phys
        psi_rows = psi.reshape(roots, bond, pairs, psi.shape[4]).transpose(0, 2, 1, 3).reshape(roots, pairs * bond, bond)
        vecs, alpha, beta = build(topo, steps, roots, bond, pairs, left_loc.shape[0])(psi_rows, left_loc, phys_loc, right_loc)
        return (vecs.reshape(roots, steps + 1, 1, phys, phys, bond), alpha[:, :, 0, 0], beta[:, :, 0, 0])

    return jax.shard_map(device_fn, mesh=mesh, in_specs=(P(), P('terms'), P('terms'), P('terms')),
                         out_specs=(P(None, None, 'terms'), P(), P()), check_vma=False)
```

```python
import functools

import jax
import jax.numpy as jnp
from jax import lax
from jax.experimental import pallas as pl
from jax.experimental.pallas import tpu as pltpu
from jax.sharding import PartitionSpec as P

LANCZOS_STEPS = 6
MESH = pl.DeviceIdType.MESH
F32 = jnp.float32
BF16 = jnp.bfloat16
PAIRS_PER_ITER = 3
SCATTER_HOOK = 3
GATHER_HOOK = 2
SEMS = 19


def lanczos_kernel(topo, steps, psi_ref, left_ref, phys_ref, right_ref, vec_ref, alpha_ref, beta_ref,
                   v, u, wide, zbuf, acc, wbuf, rc, rr, rp, beta_prev, send_sem, recv_sem):
    n = topo
    roots, rows, bond = psi_ref.shape
    pairs = rows // bond
    n_elems = rows * bond
    terms = left_ref.shape[0]
    plane = n * n
    half = pairs // 2
    quarter = half // 2
    strip = bond // plane
    me = lax.axis_index('terms')
    c = lax.rem(me, 2)
    x = lax.rem(me // 2, n)
    y = lax.rem(me // (2 * n), n)
    z = me // (2 * n * n)

    def device(zz, yy, xx, cc):
        return ((zz * n + yy) * n + xx) * 2 + cc

    sibling = device(z, y, x, 1 - c)

    ring_at = (x, y)
    plane_at = (y * n + z, z * n + x)

    def ring_peer(p, d):
        if p == 0:
            coord = lax.rem(x + d, n)
            return device(z, y, coord, c), coord
        coord = lax.rem(y + d, n)
        return device(z, coord, x, c), coord

    def plane_peer(p, e):
        d0, d1 = e // n, e % n
        if p == 0:
            yy, zz = lax.rem(y + d0, n), lax.rem(z + d1, n)
            return device(zz, yy, x, c), yy * n + zz
        zz, xx = lax.rem(z + d0, n), lax.rem(x + d1, n)
        return device(zz, y, xx, c), zz * n + xx

    def remote(src, dst, r, s, dev):
        return pltpu.make_async_remote_copy(src_ref=src, dst_ref=dst, send_sem=send_sem.at[r, s], recv_sem=recv_sem.at[r, s],
                                            device_id=(dev,), device_id_type=MESH)

    def own_q(p):
        return c * half + p * quarter + ring_at[p]

    def strip_of(m):
        return pl.ds(pl.multiple_of(m * strip, 8), strip)

    def core_scatter(r, p):
        return remote(acc.at[r, pl.ds((1 - c) * half + p * quarter, quarter)], rc.at[r, p], r, p, sibling)

    def ring_scatter(r, p):
        out = []
        for d in range(1, n):
            dev, coord = ring_peer(p, d)
            out.append(remote(acc.at[r, c * half + p * quarter + coord], rr.at[r, p, d - 1], r, 2 + 3 * p + d - 1, dev))
        return out

    def plane_scatter(r, p):
        out = []
        for e in range(1, plane):
            dev, m = plane_peer(p, e)
            out.append(remote(acc.at[r, own_q(p), strip_of(m)], rp.at[r, p, e - 1], r, 8 + p, dev))
        return out

    def plane_gather(r, p):
        out = []
        for e in range(1, plane):
            dev, _ = plane_peer(p, e)
            block = wbuf.at[r, own_q(p), strip_of(plane_at[p])]
            out.append(remote(block, block, r, 10 + p, dev))
        return out

    def plane_total(r, s, p):
        return remote(rp.at[r, p], rp.at[r, p], r, s + p, sibling)

    def ring_gather(r, p):
        out = []
        for d in range(1, n):
            dev, _ = ring_peer(p, d)
            block = wbuf.at[r, own_q(p)]
            out.append(remote(block, block, r, 12 + 3 * p + d - 1, dev))
        return out

    def core_gather(r, q):
        block = wbuf.at[r, q]
        return remote(block, block, r, 18, sibling)

    def core_total(r):
        block = wbuf.at[r, pl.ds(c * half, half)]
        return remote(block, block, r, 18, sibling)

    barrier = pltpu.get_barrier_semaphore()
    peers = [sibling] + [plane_peer(0, e)[0] for e in range(1, plane)]
    peers += [plane_peer(1, e)[0] for e in range(1, plane) if e % n]
    for dev in peers:
        pl.semaphore_signal(barrier, inc=1, device_id=(dev,), device_id_type=MESH)
    pl.semaphore_wait(barrier, len(peers))

    big = pairs * 16
    spread = jnp.where(lax.broadcasted_iota(jnp.int32, (big, pairs), 0) // 16
                       == lax.broadcasted_iota(jnp.int32, (big, pairs), 1), 1.0, 0.0).astype(BF16)
    spread_t = jnp.where(lax.broadcasted_iota(jnp.int32, (pairs, big), 1) // 16
                         == lax.broadcasted_iota(jnp.int32, (pairs, big), 0), 1.0, 0.0).astype(BF16)
    diagonal = (lax.rem(lax.broadcasted_iota(jnp.int32, (big, big), 0), 16)
                == lax.rem(lax.broadcasted_iota(jnp.int32, (big, big), 1), 16))

    def expand(i, carry):
        talls = [jnp.dot(spread, phys_ref[4 * i + k], preferred_element_type=F32).astype(BF16) for k in range(4)]
        for k in range(4):
            full = jnp.dot(talls[k], spread_t, preferred_element_type=F32)
            wide[4 * i + k] = jnp.where(diagonal, full, 0.0).astype(BF16)
        return carry

    lax.fori_loop(0, terms // 4, expand, 0)

    chunk = 2 * bond
    chunks = rows // chunk

    def rows_of(i):
        return pl.ds(pl.multiple_of(i * chunk, 8), chunk)

    def fold(t):
        return jnp.sum(t.reshape(chunk // 8, 8, bond), axis=0)

    def total(t):
        return jnp.sum(t, axis=(0, 1), keepdims=True)

    zero_tile = jnp.zeros((8, bond), F32)

    def put_vector(r, nxt, i, part):
        v[r, nxt, rows_of(i), :] = part
        small = part.astype(BF16)
        for h in range(2):
            for g in range(bond // 16):
                u[r, g, 2 * i + h] = small[h * bond + g * 16:h * bond + (g + 1) * 16]

    def put_row(r, nxt, j):
        vec_ref[r, j] = v[r, nxt, pl.ds(me, pairs, stride=bond), :]

    def first_vector(r, carry):
        def norm_body(i, s):
            part = psi_ref[r, rows_of(i), :]
            return s + fold(part * part)

        norm = jnp.sqrt(total(lax.fori_loop(0, chunks, norm_body, zero_tile)) / n_elems)

        def scale_body(i, s):
            cols = [psi_ref[r, pl.ds(2 * i + h, bond, stride=pairs), :] for h in range(2)]
            put_vector(r, 0, i, jnp.concatenate(cols, axis=0) / norm)
            v[r, 1, rows_of(i), :] = jnp.zeros((chunk, bond), F32)
            return s

        lax.fori_loop(0, chunks, scale_body, 0)
        beta_prev[r] = zero_tile
        put_row(r, 0, 0)
        return carry

    lax.fori_loop(0, roots, first_vector, 0)

    def update(r, j):
        cur, nxt = lax.rem(j, 2), lax.rem(j + 1, 2)

        def sigma(i):
            return wbuf[r, pl.ds(2 * i, 2)].reshape(chunk, bond)

        def alpha_body(i, s):
            return s + fold(sigma(i) * v[r, cur, rows_of(i), :])

        alpha = total(lax.fori_loop(0, chunks, alpha_body, zero_tile, unroll=2)) / n_elems
        before = beta_prev[r][0:1, 0:1]

        def residual_body(i, s):
            res = sigma(i) - alpha * v[r, cur, rows_of(i), :] - before * v[r, nxt, rows_of(i), :]
            wbuf[r, pl.ds(2 * i, 2)] = res.reshape(2, bond, bond)
            return s + fold(res * res)

        beta = jnp.sqrt(total(lax.fori_loop(0, chunks, residual_body, zero_tile, unroll=2)) / n_elems)

        def next_body(i, s):
            put_vector(r, nxt, i, sigma(i) / beta)
            return s

        lax.fori_loop(0, chunks, next_body, 0)
        alpha_ref[r, j] = jnp.broadcast_to(alpha, (8, bond))
        beta_ref[r, j] = jnp.broadcast_to(beta, (8, bond))
        beta_prev[r] = jnp.broadcast_to(beta, (8, bond))
        put_row(r, nxt, j + 1)

    def right_mid(r, first):
        units = [(pp, g2) for pp in range(PAIRS_PER_ITER) for g2 in range(bond // 32)]
        weights = [jnp.concatenate([right_ref[2 * (first + pp)], right_ref[2 * (first + pp) + 1]], axis=1)
                   for pp in range(PAIRS_PER_ITER)]

        def right(unit):
            pp, g2 = unit
            return [jnp.dot(u[r, g].reshape(big, bond), weights[pp], preferred_element_type=F32).astype(BF16)
                    for g in (2 * g2, 2 * g2 + 1)]

        def mid(unit, ys):
            pp, g2 = unit
            for k in range(2):
                rhs = jnp.concatenate([t[:, k * bond:(k + 1) * bond] for t in ys], axis=1)
                term = 2 * (first + pp) + k
                out = jnp.dot(wide[term], rhs, preferred_element_type=F32).astype(BF16)
                for h in range(2):
                    g = 2 * g2 + h
                    zbuf[term, :, g * 16:(g + 1) * 16, :] = out[:, h * bond:(h + 1) * bond].reshape(pairs, 16, bond)

        ys = right(units[0])
        for i, unit in enumerate(units):
            after = right(units[i + 1]) if i + 1 < len(units) else None
            mid(unit, ys)
            ys = after

    def left(r, q0):
        lhs = jnp.concatenate([left_ref[k] for k in range(terms)], axis=1)
        for qp in range(quarter // 2):
            q = q0 + 2 * qp
            cols = [jnp.concatenate([zbuf[k, q + h] for k in range(terms)], axis=0) for h in range(2)]
            out = jnp.dot(lhs, jnp.concatenate(cols, axis=1), preferred_element_type=F32)
            for h in range(2):
                acc[r, q + h] = out[:, h * bond:(h + 1) * bond]

    def start_ring(r, p):
        core_scatter(r, p).wait()
        for i in range(quarter):
            q = c * half + p * quarter + i
            acc[r, q] = acc[r, q] + rc[r, p, i]
        for copy in ring_scatter(r, p):
            copy.start()

    def ring_to_plane(r):
        for p in range(2):
            for copy in ring_scatter(r, p):
                copy.wait()
            acc[r, own_q(p)] = acc[r, own_q(p)] + rr[r, p, 0] + rr[r, p, 1] + rr[r, p, 2]
            for copy in plane_scatter(r, p):
                copy.start()

    def plane_to_gather(r):
        for p in range(2):
            done = plane_total(r, 8, p)
            done.wait_send()
            done.wait_recv()
            at = strip_of(plane_at[p])
            sums = [acc[r, own_q(p), at, :]] + [rp[r, p, e] for e in range(plane - 1)]
            while len(sums) > 1:
                sums = [a + b for a, b in zip(sums[::2], sums[1::2])]
            wbuf[r, own_q(p), at, :] = sums[0]
            for copy in plane_gather(r, p):
                copy.start()

    def plane_to_ring(r):
        for p in range(2):
            done = plane_total(r, 10, p)
            done.wait_send()
            done.wait_recv()
            for copy in ring_gather(r, p):
                copy.start()
            core_gather(r, own_q(p)).start()

    def finish_gather(r):
        for d in (1, 3, 2):
            for p in range(2):
                copy = ring_gather(r, p)[d - 1]
                copy.wait_send()
                copy.wait_recv()
                back = lax.rem(ring_at[p] + n - d, n)
                core_gather(r, c * half + p * quarter + back).start()
        done = core_total(r)
        done.wait_send()
        done.wait_recv()

    slots = roots * steps

    def slot(s, carry):
        r = lax.rem(s, roots)
        r1 = lax.rem(s + roots - 1, roots)
        r2 = lax.rem(s + roots - 2, roots)
        computing = s < slots
        scattering = jnp.logical_and(s >= 1, s < slots + 1)
        gathering = s >= 2

        def step(i, t):
            @pl.when(jnp.logical_and(gathering, i == GATHER_HOOK))
            def _():
                plane_to_ring(r2)

            @pl.when(jnp.logical_and(scattering, i == SCATTER_HOOK))
            def _():
                ring_to_plane(r1)

            @pl.when(computing)
            def _():
                right_mid(r, i * PAIRS_PER_ITER)
            return t

        lax.fori_loop(0, terms // 2 // PAIRS_PER_ITER, step, 0)

        @pl.when(computing)
        def _():
            for p in range(2):
                left(r, (1 - c) * half + p * quarter)
                core_scatter(r, p).start()
            for p in range(2):
                left(r, c * half + p * quarter)
                start_ring(r, p)

        @pl.when(scattering)
        def _():
            plane_to_gather(r1)

        @pl.when(gathering)
        def _():
            finish_gather(r2)
            update(r2, (s - 2) // roots)
        return carry

    lax.fori_loop(0, slots + 2, slot, 0)


def build(n, steps, roots, bond, pairs, terms):
    rows = pairs * bond
    half, quarter, plane = pairs // 2, pairs // 4, n * n
    vm = pl.BlockSpec(memory_space=pltpu.VMEM)
    return pl.pallas_call(
        functools.partial(lanczos_kernel, n, steps),
        out_shape=(jax.ShapeDtypeStruct((roots, steps + 1, pairs, bond), F32),
                   jax.ShapeDtypeStruct((roots, steps, 8, bond), F32),
                   jax.ShapeDtypeStruct((roots, steps, 8, bond), F32)),
        in_specs=[vm] * 4,
        out_specs=(vm, vm, vm),
        scratch_shapes=[
            pltpu.VMEM((roots, 2, rows, bond), F32),
            pltpu.VMEM((roots, bond // 16, pairs, 16, bond), BF16),
            pltpu.VMEM((terms, pairs * 16, pairs * 16), BF16),
            pltpu.VMEM((terms, pairs, bond, bond), BF16),
            pltpu.VMEM((roots, pairs, bond, bond), F32),
            pltpu.VMEM((roots, pairs, bond, bond), F32),
            pltpu.VMEM((roots, 2, quarter, bond, bond), F32),
            pltpu.VMEM((roots, 2, n - 1, bond, bond), F32),
            pltpu.VMEM((roots, 2, plane - 1, bond // plane, bond), F32),
            pltpu.VMEM((roots, 8, bond), F32),
            pltpu.SemaphoreType.DMA((roots, SEMS)),
            pltpu.SemaphoreType.DMA((roots, SEMS)),
        ],
        compiler_params=pltpu.CompilerParams(collective_id=0, has_side_effects=True,
                                             vmem_limit_bytes=60 * 1024 * 1024),
        name='lanczos',
    )


def solution(mesh):
    def device_fn(psi, left_loc, phys_loc, right_loc):
        roots, bond, phys = psi.shape[0], psi.shape[1], psi.shape[2]
        pairs = phys * phys
        vecs, alpha, beta = build(4, LANCZOS_STEPS, roots, bond, pairs, left_loc.shape[0])(
            psi.reshape(roots, bond * pairs, bond), left_loc, phys_loc, right_loc)
        return (vecs.reshape(roots, LANCZOS_STEPS + 1, 1, phys, phys, bond), alpha[:, :, 0, 0], beta[:, :, 0, 0])

    return jax.shard_map(device_fn, mesh=mesh, in_specs=(P(), P('terms'), P('terms'), P('terms')),
                         out_specs=(P(None, None, 'terms'), P(), P()), check_vma=False)
```

```python
import functools

import jax
import jax.numpy as jnp
from jax import lax
from jax.experimental import pallas as pl
from jax.experimental.pallas import tpu as pltpu
from jax.sharding import PartitionSpec as P

LANCZOS_STEPS = 6
MESH = pl.DeviceIdType.MESH
F32 = jnp.float32
BF16 = jnp.bfloat16
PAIRS_PER_ITER = 3
RING_SCATTER_AT, PLANE_SCATTER_AT, PLANE_GATHER_AT, RING_GATHER_AT = 2, 7, 2, 7
SEMS = 19


def lanczos_kernel(topo, steps, psi_ref, left_ref, phys_ref, right_ref, vec_ref, alpha_ref, beta_ref,
                   v, u, wide, zbuf, acc, wbuf, rc, rr, rp, beta_prev, send_sem, recv_sem):
    n = topo
    roots, rows, bond = psi_ref.shape
    pairs = rows // bond
    n_elems = rows * bond
    terms = left_ref.shape[0]
    plane = n * n
    half = pairs // 2
    quarter = half // 2
    strip = bond // plane
    me = lax.axis_index('terms')
    c = lax.rem(me, 2)
    x = lax.rem(me // 2, n)
    y = lax.rem(me // (2 * n), n)
    z = me // (2 * n * n)

    def device(zz, yy, xx, cc):
        return ((zz * n + yy) * n + xx) * 2 + cc

    sibling = device(z, y, x, 1 - c)

    ring_at = (x, y)
    plane_at = (y * n + z, z * n + x)

    def ring_peer(p, d):
        if p == 0:
            coord = lax.rem(x + d, n)
            return device(z, y, coord, c), coord
        coord = lax.rem(y + d, n)
        return device(z, coord, x, c), coord

    def plane_peer(p, e):
        d0, d1 = e // n, e % n
        if p == 0:
            yy, zz = lax.rem(y + d0, n), lax.rem(z + d1, n)
            return device(zz, yy, x, c), yy * n + zz
        zz, xx = lax.rem(z + d0, n), lax.rem(x + d1, n)
        return device(zz, y, xx, c), zz * n + xx

    def remote(src, dst, r, s, dev):
        return pltpu.make_async_remote_copy(src_ref=src, dst_ref=dst, send_sem=send_sem.at[r, s], recv_sem=recv_sem.at[r, s],
                                            device_id=(dev,), device_id_type=MESH)

    def own_q(p):
        return c * half + p * quarter + ring_at[p]

    def strip_of(m):
        return pl.ds(pl.multiple_of(m * strip, 8), strip)

    def core_scatter(r, p):
        return remote(acc.at[r, pl.ds((1 - c) * half + p * quarter, quarter)], rc.at[r, p], r, p, sibling)

    def ring_scatter(r, p):
        out = []
        for d in range(1, n):
            dev, coord = ring_peer(p, d)
            out.append(remote(acc.at[r, c * half + p * quarter + coord], rr.at[r, p, d - 1], r, 2 + 3 * p + d - 1, dev))
        return out

    order = sorted(range(1, plane), key=lambda e: -min(e // n, n - e // n) - min(e % n, n - e % n))

    def plane_scatter(r, p):
        out = []
        for e in order:
            dev, m = plane_peer(p, e)
            out.append(remote(acc.at[r, own_q(p), strip_of(m)], rp.at[r, p, e - 1], r, 8 + p, dev))
        return out

    def plane_gather(r, p):
        out = []
        for e in order:
            dev, _ = plane_peer(p, e)
            block = wbuf.at[r, own_q(p), strip_of(plane_at[p])]
            out.append(remote(block, block, r, 10 + p, dev))
        return out

    def plane_total(r, s, p):
        return remote(rp.at[r, p], rp.at[r, p], r, s + p, sibling)

    def ring_gather(r, p):
        out = []
        for d in range(1, n):
            dev, _ = ring_peer(p, d)
            block = wbuf.at[r, own_q(p)]
            out.append(remote(block, block, r, 12 + 3 * p + d - 1, dev))
        return out

    def core_gather(r, q):
        block = wbuf.at[r, q]
        return remote(block, block, r, 18, sibling)

    def core_total(r):
        block = wbuf.at[r, pl.ds(c * half, half)]
        return remote(block, block, r, 18, sibling)

    barrier = pltpu.get_barrier_semaphore()
    peers = [sibling] + [plane_peer(0, e)[0] for e in range(1, plane)]
    peers += [plane_peer(1, e)[0] for e in range(1, plane) if e % n]
    for dev in peers:
        pl.semaphore_signal(barrier, inc=1, device_id=(dev,), device_id_type=MESH)

    big = pairs * 16
    spread = jnp.where(lax.broadcasted_iota(jnp.int32, (big, pairs), 0) // 16
                       == lax.broadcasted_iota(jnp.int32, (big, pairs), 1), 1.0, 0.0).astype(BF16)
    spread_t = jnp.where(lax.broadcasted_iota(jnp.int32, (pairs, big), 1) // 16
                         == lax.broadcasted_iota(jnp.int32, (pairs, big), 0), 1.0, 0.0).astype(BF16)
    diagonal = (lax.rem(lax.broadcasted_iota(jnp.int32, (big, big), 0), 16)
                == lax.rem(lax.broadcasted_iota(jnp.int32, (big, big), 1), 16))

    def expand(i, carry):
        talls = [jnp.dot(spread, phys_ref[4 * i + k], preferred_element_type=F32).astype(BF16) for k in range(4)]
        for k in range(4):
            full = jnp.dot(talls[k], spread_t, preferred_element_type=F32)
            wide[4 * i + k] = jnp.where(diagonal, full, 0.0).astype(BF16)
        return carry

    lax.fori_loop(0, terms // 4, expand, 0)

    chunk = 2 * bond
    chunks = rows // chunk

    def rows_of(i):
        return pl.ds(pl.multiple_of(i * chunk, 8), chunk)

    def fold(t):
        return jnp.sum(t.reshape(chunk // 8, 8, bond), axis=0)

    def total(t):
        return jnp.sum(t, axis=(0, 1), keepdims=True)

    zero_tile = jnp.zeros((8, bond), F32)

    def put_vector(r, nxt, i, part):
        v[r, nxt, rows_of(i), :] = part
        small = part.astype(BF16)
        for h in range(2):
            for g in range(bond // 16):
                u[r, g, 2 * i + h] = small[h * bond + g * 16:h * bond + (g + 1) * 16]

    def put_row(r, nxt, j):
        vec_ref[r, j] = v[r, nxt, pl.ds(me, pairs, stride=bond), :]

    def first_vector(r, carry):
        def norm_body(i, s):
            part = psi_ref[r, rows_of(i), :]
            return s + fold(part * part)

        norm = jnp.sqrt(total(lax.fori_loop(0, chunks, norm_body, zero_tile)) / n_elems)

        def scale_body(i, s):
            cols = [psi_ref[r, pl.ds(2 * i + h, bond, stride=pairs), :] for h in range(2)]
            put_vector(r, 0, i, jnp.concatenate(cols, axis=0) / norm)
            v[r, 1, rows_of(i), :] = jnp.zeros((chunk, bond), F32)
            return s

        lax.fori_loop(0, chunks, scale_body, 0)
        beta_prev[r] = zero_tile
        put_row(r, 0, 0)
        return carry

    lax.fori_loop(0, roots, first_vector, 0)
    pl.semaphore_wait(barrier, len(peers))

    def update(r, j):
        cur, nxt = lax.rem(j, 2), lax.rem(j + 1, 2)

        def sigma(i):
            return wbuf[r, pl.ds(2 * i, 2)].reshape(chunk, bond)

        def alpha_body(i, s):
            return s + fold(sigma(i) * v[r, cur, rows_of(i), :])

        alpha = total(lax.fori_loop(0, chunks, alpha_body, zero_tile, unroll=2)) / n_elems
        before = beta_prev[r][0:1, 0:1]

        def residual_body(i, s):
            res = sigma(i) - alpha * v[r, cur, rows_of(i), :] - before * v[r, nxt, rows_of(i), :]
            wbuf[r, pl.ds(2 * i, 2)] = res.reshape(2, bond, bond)
            return s + fold(res * res)

        beta = jnp.sqrt(total(lax.fori_loop(0, chunks, residual_body, zero_tile, unroll=2)) / n_elems)

        def next_body(i, s):
            put_vector(r, nxt, i, sigma(i) / beta)
            return s

        lax.fori_loop(0, chunks, next_body, 0)
        alpha_ref[r, j] = alpha[0, 0]
        beta_ref[r, j] = beta[0, 0]
        beta_prev[r] = jnp.broadcast_to(beta, (8, bond))
        put_row(r, nxt, j + 1)

    def right_mid(r, first):
        units = [(pp, g2) for pp in range(PAIRS_PER_ITER) for g2 in range(bond // 32)]
        weights = [jnp.concatenate([right_ref[2 * (first + pp)], right_ref[2 * (first + pp) + 1]], axis=1)
                   for pp in range(PAIRS_PER_ITER)]

        def right(unit):
            pp, g2 = unit
            return [jnp.dot(u[r, g].reshape(big, bond), weights[pp], preferred_element_type=F32).astype(BF16)
                    for g in (2 * g2, 2 * g2 + 1)]

        def mid(unit, ys):
            pp, g2 = unit
            for k in range(2):
                rhs = jnp.concatenate([t[:, k * bond:(k + 1) * bond] for t in ys], axis=1)
                term = 2 * (first + pp) + k
                out = jnp.dot(wide[term], rhs, preferred_element_type=F32).astype(BF16)
                for h in range(2):
                    g = 2 * g2 + h
                    zbuf[term, :, g * 16:(g + 1) * 16, :] = out[:, h * bond:(h + 1) * bond].reshape(pairs, 16, bond)

        ys = right(units[0])
        for i, unit in enumerate(units):
            after = right(units[i + 1]) if i + 1 < len(units) else None
            mid(unit, ys)
            ys = after

    def left(r, q0):
        lhs = jnp.concatenate([left_ref[k] for k in range(terms)], axis=1)
        for qp in range(quarter // 2):
            q = q0 + 2 * qp
            cols = [jnp.concatenate([zbuf[k, q + h] for k in range(terms)], axis=0) for h in range(2)]
            out = jnp.dot(lhs, jnp.concatenate(cols, axis=1), preferred_element_type=F32)
            for h in range(2):
                acc[r, q + h] = out[:, h * bond:(h + 1) * bond]

    def start_ring(r):
        for p in range(2):
            core_scatter(r, p).wait()
            for i in range(quarter):
                q = c * half + p * quarter + i
                acc[r, q] = acc[r, q] + rc[r, p, i]
        both = [ring_scatter(r, p) for p in range(2)]
        for d in (2, 1, 3):
            for p in range(2):
                both[p][d - 1].start()

    def ring_to_plane(r):
        for p in range(2):
            for copy in ring_scatter(r, p):
                copy.wait()
            acc[r, own_q(p)] = acc[r, own_q(p)] + rr[r, p, 0] + rr[r, p, 1] + rr[r, p, 2]
            for copy in plane_scatter(r, p):
                copy.start()

    def plane_to_gather(r):
        for p in range(2):
            done = plane_total(r, 8, p)
            done.wait_send()
            done.wait_recv()
            at = strip_of(plane_at[p])
            sums = [acc[r, own_q(p), at, :]] + [rp[r, p, e] for e in range(plane - 1)]
            while len(sums) > 1:
                sums = [a + b for a, b in zip(sums[::2], sums[1::2])]
            wbuf[r, own_q(p), at, :] = sums[0]
            for copy in plane_gather(r, p):
                copy.start()

    def plane_to_ring(r):
        for p in range(2):
            done = plane_total(r, 10, p)
            done.wait_send()
            done.wait_recv()
        both = [ring_gather(r, p) for p in range(2)]
        for d in (2, 1, 3):
            for p in range(2):
                both[p][d - 1].start()
        for p in range(2):
            core_gather(r, own_q(p)).start()

    def ring_to_core(r):
        for d in (1, 3, 2):
            for p in range(2):
                copy = ring_gather(r, p)[d - 1]
                copy.wait_send()
                copy.wait_recv()
                back = lax.rem(ring_at[p] + n - d, n)
                core_gather(r, c * half + p * quarter + back).start()

    def finish_gather(r):
        done = core_total(r)
        done.wait_send()
        done.wait_recv()

    RM_STEPS = terms // 2 // PAIRS_PER_ITER
    PLACES = (RING_SCATTER_AT, PLANE_SCATTER_AT, PLANE_GATHER_AT, RING_GATHER_AT)
    slots = roots * steps

    def slot(s, carry):
        r = lax.rem(s, roots)
        r1 = lax.rem(s + roots - 1, roots)
        r2 = lax.rem(s + roots - 2, roots)
        computing = s < slots
        scattering = jnp.logical_and(s >= 1, s < slots + 1)
        gathering = s >= 2

        def hooks(at, here):
            for place, guard, root, work in ((RING_SCATTER_AT, scattering, r1, ring_to_plane),
                                             (PLANE_GATHER_AT, gathering, r2, plane_to_ring),
                                             (PLANE_SCATTER_AT, scattering, r1, plane_to_gather),
                                             (RING_GATHER_AT, gathering, r2, ring_to_core)):
                if place in here:
                    pl.when(jnp.logical_and(guard, at == place))(functools.partial(work, root))

        def step(i, t):
            hooks(i, range(RM_STEPS))

            @pl.when(computing)
            def _():
                right_mid(r, i * PAIRS_PER_ITER)
            return t

        lax.fori_loop(0, RM_STEPS, step, 0)

        def left_part(k):
            p = k % 2
            if k < 2:
                left(r, (1 - c) * half + p * quarter)
                core_scatter(r, p).start()
            else:
                left(r, c * half + p * quarter)
                if k == 3:
                    start_ring(r)

        group = []
        for k in range(4):
            if RM_STEPS + k in PLACES and group:
                pl.when(computing)(functools.partial(lambda ks: [left_part(m) for m in ks] and None, group))
                group = []
            hooks(RM_STEPS + k, (RM_STEPS + k,))
            group.append(k)
        pl.when(computing)(functools.partial(lambda ks: [left_part(m) for m in ks] and None, group))
        hooks(RM_STEPS + 4, (RM_STEPS + 4,))

        @pl.when(gathering)
        def _():
            finish_gather(r2)
            update(r2, (s - 2) // roots)
        return carry

    lax.fori_loop(0, slots + 2, slot, 0)


def build(n, steps, roots, bond, pairs, terms):
    rows = pairs * bond
    half, quarter, plane = pairs // 2, pairs // 4, n * n
    vm = pl.BlockSpec(memory_space=pltpu.VMEM)
    return pl.pallas_call(
        functools.partial(lanczos_kernel, n, steps),
        out_shape=(jax.ShapeDtypeStruct((roots, steps + 1, pairs, bond), F32),
                   jax.ShapeDtypeStruct((roots, steps), F32), jax.ShapeDtypeStruct((roots, steps), F32)),
        in_specs=[vm] * 4,
        out_specs=(vm, pl.BlockSpec(memory_space=pltpu.SMEM), pl.BlockSpec(memory_space=pltpu.SMEM)),
        scratch_shapes=[
            pltpu.VMEM((roots, 2, rows, bond), F32),
            pltpu.VMEM((roots, bond // 16, pairs, 16, bond), BF16),
            pltpu.VMEM((terms, pairs * 16, pairs * 16), BF16),
            pltpu.VMEM((terms, pairs, bond, bond), BF16),
            pltpu.VMEM((roots, pairs, bond, bond), F32),
            pltpu.VMEM((roots, pairs, bond, bond), F32),
            pltpu.VMEM((roots, 2, quarter, bond, bond), F32),
            pltpu.VMEM((roots, 2, n - 1, bond, bond), F32),
            pltpu.VMEM((roots, 2, plane - 1, bond // plane, bond), F32),
            pltpu.VMEM((roots, 8, bond), F32),
            pltpu.SemaphoreType.DMA((roots, SEMS)),
            pltpu.SemaphoreType.DMA((roots, SEMS)),
        ],
        compiler_params=pltpu.CompilerParams(collective_id=0, has_side_effects=True,
                                             vmem_limit_bytes=60 * 1024 * 1024),
        name='lanczos',
    )


def solution(mesh):
    def device_fn(psi, left_loc, phys_loc, right_loc):
        roots, bond, phys = psi.shape[0], psi.shape[1], psi.shape[2]
        pairs = phys * phys
        vecs, alpha, beta = build(4, LANCZOS_STEPS, roots, bond, pairs, left_loc.shape[0])(
            psi.reshape(roots, bond * pairs, bond), left_loc, phys_loc, right_loc)
        return (vecs.reshape(roots, LANCZOS_STEPS + 1, 1, phys, phys, bond), alpha, beta)

    return jax.shard_map(device_fn, mesh=mesh, in_specs=(P(), P('terms'), P('terms'), P('terms')),
                         out_specs=(P(None, None, 'terms'), P(), P()), check_vma=False)
```

```python
import functools

import jax
import jax.numpy as jnp
from jax import lax
from jax.experimental import pallas as pl
from jax.experimental.pallas import tpu as pltpu
from jax.sharding import PartitionSpec as P

LANCZOS_STEPS = 6
MESH = pl.DeviceIdType.MESH
F32 = jnp.float32
BF16 = jnp.bfloat16
PAIRS_PER_ITER = 3
RING_SCATTER_AT, PLANE_SCATTER_AT, PLANE_GATHER_AT, RING_GATHER_AT = 2, 7, 2, 7
SEMS = 19


def lanczos_kernel(topo, steps, psi_ref, left_ref, phys_ref, right_ref, vec_ref, alpha_ref, beta_ref,
                   v, u, wide, zbuf, acc, wbuf, rc, rr, rp, beta_prev, send_sem, recv_sem):
    n = topo
    roots, rows, bond = psi_ref.shape
    pairs = rows // bond
    n_elems = rows * bond
    terms = left_ref.shape[0]
    plane = n * n
    half = pairs // 2
    quarter = half // 2
    strip = bond // plane
    me = lax.axis_index('terms')
    c = lax.rem(me, 2)
    x = lax.rem(me // 2, n)
    y = lax.rem(me // (2 * n), n)
    z = me // (2 * n * n)

    def device(zz, yy, xx, cc):
        return ((zz * n + yy) * n + xx) * 2 + cc

    sibling = device(z, y, x, 1 - c)

    ring_at = (x, y)
    plane_at = (y * n + z, z * n + x)

    def ring_peer(p, d):
        if p == 0:
            coord = lax.rem(x + d, n)
            return device(z, y, coord, c), coord
        coord = lax.rem(y + d, n)
        return device(z, coord, x, c), coord

    def plane_peer(p, e):
        d0, d1 = e // n, e % n
        if p == 0:
            yy, zz = lax.rem(y + d0, n), lax.rem(z + d1, n)
            return device(zz, yy, x, c), yy * n + zz
        zz, xx = lax.rem(z + d0, n), lax.rem(x + d1, n)
        return device(zz, y, xx, c), zz * n + xx

    def remote(src, dst, r, s, dev):
        return pltpu.make_async_remote_copy(src_ref=src, dst_ref=dst, send_sem=send_sem.at[r, s], recv_sem=recv_sem.at[r, s],
                                            device_id=(dev,), device_id_type=MESH)

    def own_q(p):
        return c * half + p * quarter + ring_at[p]

    def strip_of(m):
        return pl.ds(pl.multiple_of(m * strip, 8), strip)

    def core_scatter(r, p):
        return remote(acc.at[r, pl.ds((1 - c) * half + p * quarter, quarter)], rc.at[r, p], r, p, sibling)

    def ring_scatter(r, p):
        out = []
        for d in range(1, n):
            dev, coord = ring_peer(p, d)
            out.append(remote(acc.at[r, c * half + p * quarter + coord], rr.at[r, p, d - 1], r, 2 + 3 * p + d - 1, dev))
        return out

    order = sorted(range(1, plane), key=lambda e: -min(e // n, n - e // n) - min(e % n, n - e % n))

    def plane_scatter(r, p):
        out = []
        for e in order:
            dev, m = plane_peer(p, e)
            out.append(remote(acc.at[r, own_q(p), strip_of(m)], rp.at[r, p, e - 1], r, 8 + p, dev))
        return out

    def plane_gather(r, p):
        out = []
        for e in order:
            dev, _ = plane_peer(p, e)
            block = wbuf.at[r, own_q(p), strip_of(plane_at[p])]
            out.append(remote(block, block, r, 10 + p, dev))
        return out

    def plane_total(r, s, p):
        return remote(rp.at[r, p], rp.at[r, p], r, s + p, sibling)

    def ring_gather(r, p):
        out = []
        for d in range(1, n):
            dev, _ = ring_peer(p, d)
            block = wbuf.at[r, own_q(p)]
            out.append(remote(block, block, r, 12 + 3 * p + d - 1, dev))
        return out

    def core_gather(r, q):
        block = wbuf.at[r, q]
        return remote(block, block, r, 18, sibling)

    def core_total(r):
        block = wbuf.at[r, pl.ds(c * half, half)]
        return remote(block, block, r, 18, sibling)

    barrier = pltpu.get_barrier_semaphore()
    peers = [sibling] + [plane_peer(0, e)[0] for e in range(1, plane)]
    peers += [plane_peer(1, e)[0] for e in range(1, plane) if e % n]
    for dev in peers:
        pl.semaphore_signal(barrier, inc=1, device_id=(dev,), device_id_type=MESH)

    big = pairs * 16
    spread = jnp.where(lax.broadcasted_iota(jnp.int32, (big, pairs), 0) // 16
                       == lax.broadcasted_iota(jnp.int32, (big, pairs), 1), 1.0, 0.0).astype(BF16)
    spread_t = jnp.where(lax.broadcasted_iota(jnp.int32, (pairs, big), 1) // 16
                         == lax.broadcasted_iota(jnp.int32, (pairs, big), 0), 1.0, 0.0).astype(BF16)
    diagonal = (lax.rem(lax.broadcasted_iota(jnp.int32, (big, big), 0), 16)
                == lax.rem(lax.broadcasted_iota(jnp.int32, (big, big), 1), 16))

    def expand(i, carry):
        talls = [jnp.dot(spread, phys_ref[4 * i + k], preferred_element_type=F32).astype(BF16) for k in range(4)]
        for k in range(4):
            full = jnp.dot(talls[k], spread_t, preferred_element_type=F32)
            wide[4 * i + k] = jnp.where(diagonal, full, 0.0).astype(BF16)
        return carry

    lax.fori_loop(0, terms // 4, expand, 0)

    chunk = 2 * bond
    chunks = rows // chunk

    def rows_of(i):
        return pl.ds(pl.multiple_of(i * chunk, 8), chunk)

    def fold(t):
        return jnp.sum(t.reshape(chunk // 8, 8, bond), axis=0)

    def total(t):
        return jnp.sum(t, axis=(0, 1), keepdims=True)

    zero_tile = jnp.zeros((8, bond), F32)

    def put_vector(r, nxt, i, part):
        v[r, nxt, rows_of(i), :] = part
        small = part.astype(BF16)
        for h in range(2):
            for g in range(bond // 16):
                u[r, g, 2 * i + h] = small[h * bond + g * 16:h * bond + (g + 1) * 16]

    def put_row(r, nxt, j):
        vec_ref[r, j] = v[r, nxt, pl.ds(me, pairs, stride=bond), :]

    def first_vector(r, carry):
        def norm_body(i, s):
            part = psi_ref[r, rows_of(i), :]
            return s + fold(part * part)

        norm = jnp.sqrt(total(lax.fori_loop(0, chunks, norm_body, zero_tile)) / n_elems)

        def scale_body(i, s):
            cols = [psi_ref[r, pl.ds(2 * i + h, bond, stride=pairs), :] for h in range(2)]
            put_vector(r, 0, i, jnp.concatenate(cols, axis=0) / norm)
            v[r, 1, rows_of(i), :] = jnp.zeros((chunk, bond), F32)
            return s

        lax.fori_loop(0, chunks, scale_body, 0)
        beta_prev[r] = zero_tile
        put_row(r, 0, 0)
        return carry

    lax.fori_loop(0, roots, first_vector, 0)
    pl.semaphore_wait(barrier, len(peers))

    def update(r, j):
        cur, nxt = lax.rem(j, 2), lax.rem(j + 1, 2)

        def sigma(i):
            return wbuf[r, pl.ds(2 * i, 2)].reshape(chunk, bond)

        def alpha_body(i, s):
            return s + fold(sigma(i) * v[r, cur, rows_of(i), :])

        def alpha_half(which):
            first = which * (chunks // 2)
            return lax.fori_loop(0, chunks // 2, lambda i, s: alpha_body(first + i, s), zero_tile)

        mine = alpha_half(c)
        finish_gather(r)
        alpha = total(mine + alpha_half(1 - c)) / n_elems
        before = beta_prev[r][0:1, 0:1]

        def residual_body(i, s):
            res = sigma(i) - alpha * v[r, cur, rows_of(i), :] - before * v[r, nxt, rows_of(i), :]
            wbuf[r, pl.ds(2 * i, 2)] = res.reshape(2, bond, bond)
            return s + fold(res * res)

        beta = jnp.sqrt(total(lax.fori_loop(0, chunks, residual_body, zero_tile, unroll=2)) / n_elems)

        def next_body(i, s):
            put_vector(r, nxt, i, sigma(i) / beta)
            return s

        lax.fori_loop(0, chunks, next_body, 0, unroll=2)
        alpha_ref[r, j] = alpha[0, 0]
        beta_ref[r, j] = beta[0, 0]
        beta_prev[r] = jnp.broadcast_to(beta, (8, bond))
        put_row(r, nxt, j + 1)

    def right_mid(r, first):
        units = [(pp, g2) for pp in range(PAIRS_PER_ITER) for g2 in range(bond // 32)]
        weights = [jnp.concatenate([right_ref[2 * (first + pp)], right_ref[2 * (first + pp) + 1]], axis=1)
                   for pp in range(PAIRS_PER_ITER)]

        def right(unit):
            pp, g2 = unit
            return [jnp.dot(u[r, g].reshape(big, bond), weights[pp], preferred_element_type=F32).astype(BF16)
                    for g in (2 * g2, 2 * g2 + 1)]

        def mid(unit, ys):
            pp, g2 = unit
            for k in range(2):
                rhs = jnp.concatenate([t[:, k * bond:(k + 1) * bond] for t in ys], axis=1)
                term = 2 * (first + pp) + k
                out = jnp.dot(wide[term], rhs, preferred_element_type=F32).astype(BF16)
                for h in range(2):
                    g = 2 * g2 + h
                    zbuf[term, :, g * 16:(g + 1) * 16, :] = out[:, h * bond:(h + 1) * bond].reshape(pairs, 16, bond)

        ys = right(units[0])
        for i, unit in enumerate(units):
            after = right(units[i + 1]) if i + 1 < len(units) else None
            mid(unit, ys)
            ys = after

    def left(r, q0):
        lhs = jnp.concatenate([left_ref[k] for k in range(terms)], axis=1)
        for qp in range(quarter // 2):
            q = q0 + 2 * qp
            cols = [jnp.concatenate([zbuf[k, q + h] for k in range(terms)], axis=0) for h in range(2)]
            out = jnp.dot(lhs, jnp.concatenate(cols, axis=1), preferred_element_type=F32)
            for h in range(2):
                acc[r, q + h] = out[:, h * bond:(h + 1) * bond]

    def start_ring(r):
        for p in range(2):
            core_scatter(r, p).wait()
            for i in range(quarter):
                q = c * half + p * quarter + i
                acc[r, q] = acc[r, q] + rc[r, p, i]
        both = [ring_scatter(r, p) for p in range(2)]
        for d in (2, 1, 3):
            for p in range(2):
                both[p][d - 1].start()

    def ring_to_plane(r):
        for p in range(2):
            for copy in ring_scatter(r, p):
                copy.wait()
            acc[r, own_q(p)] = acc[r, own_q(p)] + rr[r, p, 0] + rr[r, p, 1] + rr[r, p, 2]
        for pair in zip(plane_scatter(r, 0), plane_scatter(r, 1)):
            for copy in pair:
                copy.start()

    def plane_to_gather(r):
        for p in range(2):
            done = plane_total(r, 8, p)
            done.wait_send()
            done.wait_recv()
            at = strip_of(plane_at[p])
            sums = [acc[r, own_q(p), at, :]] + [rp[r, p, e] for e in range(plane - 1)]
            while len(sums) > 1:
                sums = [a + b for a, b in zip(sums[::2], sums[1::2])]
            wbuf[r, own_q(p), at, :] = sums[0]
        for pair in zip(plane_gather(r, 0), plane_gather(r, 1)):
            for copy in pair:
                copy.start()

    def plane_to_ring(r):
        for p in range(2):
            done = plane_total(r, 10, p)
            done.wait_send()
            done.wait_recv()
        both = [ring_gather(r, p) for p in range(2)]
        for d in (2, 1, 3):
            for p in range(2):
                both[p][d - 1].start()
        for p in range(2):
            core_gather(r, own_q(p)).start()

    def ring_to_core(r):
        for d in (1, 3, 2):
            for p in range(2):
                copy = ring_gather(r, p)[d - 1]
                copy.wait_send()
                copy.wait_recv()
                back = lax.rem(ring_at[p] + n - d, n)
                core_gather(r, c * half + p * quarter + back).start()

    def finish_gather(r):
        done = core_total(r)
        done.wait_send()
        done.wait_recv()

    RM_STEPS = terms // 2 // PAIRS_PER_ITER
    PLACES = (RING_SCATTER_AT, PLANE_SCATTER_AT, PLANE_GATHER_AT, RING_GATHER_AT)
    slots = roots * steps

    def slot(s, carry):
        r = lax.rem(s, roots)
        r1 = lax.rem(s + roots - 1, roots)
        r2 = lax.rem(s + roots - 2, roots)
        computing = s < slots
        scattering = jnp.logical_and(s >= 1, s < slots + 1)
        gathering = s >= 2

        def hooks(at, here):
            for place, guard, root, work in ((RING_SCATTER_AT, scattering, r1, ring_to_plane),
                                             (PLANE_GATHER_AT, gathering, r2, plane_to_ring),
                                             (PLANE_SCATTER_AT, scattering, r1, plane_to_gather),
                                             (RING_GATHER_AT, gathering, r2, ring_to_core)):
                if place in here:
                    pl.when(jnp.logical_and(guard, at == place))(functools.partial(work, root))

        def step(i, t):
            hooks(i, range(RM_STEPS))

            @pl.when(computing)
            def _():
                right_mid(r, i * PAIRS_PER_ITER)
            return t

        lax.fori_loop(0, RM_STEPS, step, 0)

        def left_part(k):
            p = k % 2
            if k < 2:
                left(r, (1 - c) * half + p * quarter)
                core_scatter(r, p).start()
            else:
                left(r, c * half + p * quarter)
                if k == 3:
                    start_ring(r)

        group = []
        for k in range(4):
            if RM_STEPS + k in PLACES and group:
                pl.when(computing)(functools.partial(lambda ks: [left_part(m) for m in ks] and None, group))
                group = []
            hooks(RM_STEPS + k, (RM_STEPS + k,))
            group.append(k)
        pl.when(computing)(functools.partial(lambda ks: [left_part(m) for m in ks] and None, group))
        hooks(RM_STEPS + 4, (RM_STEPS + 4,))

        @pl.when(gathering)
        def _():
            update(r2, (s - 2) // roots)
        return carry

    lax.fori_loop(0, slots + 2, slot, 0)


def build(n, steps, roots, bond, pairs, terms):
    rows = pairs * bond
    half, quarter, plane = pairs // 2, pairs // 4, n * n
    vm = pl.BlockSpec(memory_space=pltpu.VMEM)
    return pl.pallas_call(
        functools.partial(lanczos_kernel, n, steps),
        out_shape=(jax.ShapeDtypeStruct((roots, steps + 1, pairs, bond), F32),
                   jax.ShapeDtypeStruct((roots, steps), F32), jax.ShapeDtypeStruct((roots, steps), F32)),
        in_specs=[vm] * 4,
        out_specs=(vm, pl.BlockSpec(memory_space=pltpu.SMEM), pl.BlockSpec(memory_space=pltpu.SMEM)),
        scratch_shapes=[
            pltpu.VMEM((roots, 2, rows, bond), F32),
            pltpu.VMEM((roots, bond // 16, pairs, 16, bond), BF16),
            pltpu.VMEM((terms, pairs * 16, pairs * 16), BF16),
            pltpu.VMEM((terms, pairs, bond, bond), BF16),
            pltpu.VMEM((roots, pairs, bond, bond), F32),
            pltpu.VMEM((roots, pairs, bond, bond), F32),
            pltpu.VMEM((roots, 2, quarter, bond, bond), F32),
            pltpu.VMEM((roots, 2, n - 1, bond, bond), F32),
            pltpu.VMEM((roots, 2, plane - 1, bond // plane, bond), F32),
            pltpu.VMEM((roots, 8, bond), F32),
            pltpu.SemaphoreType.DMA((roots, SEMS)),
            pltpu.SemaphoreType.DMA((roots, SEMS)),
        ],
        compiler_params=pltpu.CompilerParams(collective_id=0, has_side_effects=True,
                                             vmem_limit_bytes=60 * 1024 * 1024),
        name='lanczos',
    )


def solution(mesh):
    def device_fn(psi, left_loc, phys_loc, right_loc):
        roots, bond, phys = psi.shape[0], psi.shape[1], psi.shape[2]
        pairs = phys * phys
        vecs, alpha, beta = build(4, LANCZOS_STEPS, roots, bond, pairs, left_loc.shape[0])(
            psi.reshape(roots, bond * pairs, bond), left_loc, phys_loc, right_loc)
        return (vecs.reshape(roots, LANCZOS_STEPS + 1, 1, phys, phys, bond), alpha, beta)

    return jax.shard_map(device_fn, mesh=mesh, in_specs=(P(), P('terms'), P('terms'), P('terms')),
                         out_specs=(P(None, None, 'terms'), P(), P()), check_vma=False)
```
